16 devices in a mesh: dp: 4 (over z, y), tp: 4 (over x, core).
Axes of the slice: x: 2, y: 2, z: 2, core: 2. Of those that a mesh axis runs over, the one named last changes fastest.
Arguments:
- x: bfloat16 [32, 128, 8192], P('dp'), parts along dimension 0
- seq_lens: int32 [32], P('dp'), parts along dimension 0
- w_query: bfloat16 [8192, 8192], P(None, 'tp')
- w_key: bfloat16 [8192, 1024], P(None, 'tp')
- w_value: bfloat16 [8192, 1024], P(None, 'tp')
- w_out: bfloat16 [8192, 8192], P('tp')
- w_gate: bfloat16 [8192, 22016], P(None, 'tp')
- w_up: bfloat16 [8192, 22016], P(None, 'tp')
- w_down: bfloat16 [22016, 8192], P('tp')
- attn_gain: bfloat16 [8192], replicated
- mlp_gain: bfloat16 [8192], replicated
- k_cache: bfloat16 [32, 256, 8, 128], P('dp', None, 'tp'), parts along dimension 0
- v_cache: bfloat16 [32, 256, 8, 128], P('dp', None, 'tp'), parts along dimension 0
Outputs:
- output 1: bfloat16 [32, 128, 8192], P('dp'), parts along dimension 0
- output 2: bfloat16 [32, 256, 8, 128], P('dp', None, 'tp'), parts along dimension 0
- output 3: bfloat16 [32, 256, 8, 128], P('dp', None, 'tp'), parts along dimension 0
There are 4 independent parts. The reference program is written for one: setup_inputs(seed, part) draws one part's arguments, and reference() takes and returns one part's arrays. A program takes and returns all parts, laid end to end along the dimension named above; an argument that names none is the same for every part.
All inputs are finite; a program needn't handle non-finite values.
Results may differ from the reference program's by a relative error of at most 0.0111989.
Values are sent between devices in bfloat16 or wider.
A program may use at most 1.5 GiB of HBM per device.

```python
import jax
import jax.numpy as jnp
from jax import lax

D = 8192
HEADS = 64
KV_HEADS = 8
HEAD = 128
FF = 22016
BATCH = 8
SEQ = 128
CACHE_LEN = 256
TP = 4
EPS = 1e-5
ROPE_BASE = 10000.0


def setup_inputs(seed: int = 0, part: int = 0) -> dict:
    base_key = jax.random.key(seed)
    part_key = jax.random.fold_in(base_key, part)
    weight_keys = jax.random.split(base_key, 9)
    part_keys = jax.random.split(part_key, 5)
    qk_scale = 1.5 * D ** -0.5

    def normal_weight(rng_key, array_shape, factor):
        return (jax.random.normal(rng_key, array_shape, jnp.float32) * factor).astype(jnp.bfloat16)

    short_len = jax.random.randint(part_keys[1], (1,), SEQ // 2, (4 * SEQ) // 5 + 1)
    other_lens = jax.random.randint(part_keys[2], (BATCH - 1,), SEQ // 2, SEQ + 1)
    return {
        "x": normal_weight(part_keys[0], (BATCH, SEQ, D), 1.0),
        "seq_lens": jnp.concatenate([short_len, other_lens]).astype(jnp.int32),
        "w_query": normal_weight(weight_keys[0], (D, HEADS * HEAD), qk_scale),
        "w_key": normal_weight(weight_keys[1], (D, KV_HEADS * HEAD), qk_scale),
        "w_value": normal_weight(weight_keys[2], (D, KV_HEADS * HEAD), D ** -0.5),
        "w_out": normal_weight(weight_keys[3], (HEADS * HEAD, D), (HEADS * HEAD) ** -0.5),
        "w_gate": normal_weight(weight_keys[4], (D, FF), D ** -0.5),
        "w_up": normal_weight(weight_keys[5], (D, FF), D ** -0.5),
        "w_down": normal_weight(weight_keys[6], (FF, D), FF ** -0.5),
        "attn_gain": jax.random.uniform(weight_keys[7], (D,), jnp.float32, 0.5, 1.5).astype(jnp.bfloat16),
        "mlp_gain": jax.random.uniform(weight_keys[8], (D,), jnp.float32, 0.5, 1.5).astype(jnp.bfloat16),
        "k_cache": normal_weight(part_keys[3], (BATCH, CACHE_LEN, KV_HEADS, HEAD), 1.0),
        "v_cache": normal_weight(part_keys[4], (BATCH, CACHE_LEN, KV_HEADS, HEAD), 1.0),
    }


def rms_norm(rows, gain):
    rows32 = rows.astype(jnp.float32)
    inv_rms = lax.rsqrt(jnp.mean(rows32 * rows32, axis=-1, keepdims=True) + EPS)
    return (rows32 * inv_rms * gain.astype(jnp.float32)).astype(jnp.bfloat16)


def rotary(vecs, angles):
    half_dim = HEAD // 2
    pairs = vecs.reshape(vecs.shape[:-1] + (half_dim, 2))
    even_part = pairs[..., 0]
    odd_part = pairs[..., 1]
    cos_tab = jnp.cos(angles)[:, None, :]
    sin_tab = jnp.sin(angles)[:, None, :]
    turned = jnp.stack([even_part * cos_tab - odd_part * sin_tab, even_part * sin_tab + odd_part * cos_tab], axis=-1)
    return turned.reshape(vecs.shape)


def reference(x, seq_lens, w_query, w_key, w_value, w_out, w_gate, w_up, w_down, attn_gain, mlp_gain, k_cache, v_cache):
    group_size = HEADS // KV_HEADS
    heads_part = HEADS * HEAD // TP
    ff_part = FF // TP
    positions = jnp.arange(SEQ)
    inv_freq = ROPE_BASE ** (-jnp.arange(0, HEAD, 2).astype(jnp.float32) / HEAD)
    angles = positions.astype(jnp.float32)[:, None] * inv_freq[None, :]
    causal = positions[None, :] <= positions[:, None]

    def one_sequence(items):
        x_row, length = items
        normed = rms_norm(x_row, attn_gain)
        queries = rotary(jnp.dot(normed, w_query, preferred_element_type=jnp.float32).reshape(SEQ, HEADS, HEAD), angles).astype(jnp.bfloat16)
        keys = rotary(jnp.dot(normed, w_key, preferred_element_type=jnp.float32).reshape(SEQ, KV_HEADS, HEAD), angles).astype(jnp.bfloat16)
        values = jnp.dot(normed, w_value, preferred_element_type=jnp.float32).astype(jnp.bfloat16).reshape(SEQ, KV_HEADS, HEAD)
        valid = positions < length
        keys = jnp.where(valid[:, None, None], keys, jnp.zeros_like(keys))
        values = jnp.where(valid[:, None, None], values, jnp.zeros_like(values))
        allowed = causal & valid[None, :]

        def one_kv_head(blocks):
            q_block, k_block, v_block = blocks
            scores = jnp.einsum("qgh,sh->gqs", q_block.astype(jnp.float32), k_block.astype(jnp.float32)) * HEAD ** -0.5
            scores = jnp.where(allowed[None], scores, -jnp.inf)
            probs = jax.nn.softmax(scores, axis=-1).astype(jnp.bfloat16)
            mixed = jnp.einsum("gqs,sh->qgh", probs.astype(jnp.float32), v_block.astype(jnp.float32))
            return mixed.astype(jnp.bfloat16)

        q_grouped = jnp.transpose(queries.reshape(SEQ, KV_HEADS, group_size, HEAD), (1, 0, 2, 3))
        head_out = lax.map(one_kv_head, (q_grouped, jnp.transpose(keys, (1, 0, 2)), jnp.transpose(values, (1, 0, 2))))
        attn_rows = jnp.transpose(head_out, (1, 0, 2, 3)).reshape(SEQ, HEADS * HEAD)
        attn_sum = jnp.zeros((SEQ, D), jnp.float32)
        for index in range(TP):
            partial = jnp.dot(attn_rows[:, index * heads_part:(index + 1) * heads_part], w_out[index * heads_part:(index + 1) * heads_part], preferred_element_type=jnp.float32)
            attn_sum = attn_sum + partial.astype(jnp.bfloat16).astype(jnp.float32)
        hidden = (x_row.astype(jnp.float32) + attn_sum).astype(jnp.bfloat16)
        normed_mlp = rms_norm(hidden, mlp_gain)
        gate_pre = jnp.dot(normed_mlp, w_gate, preferred_element_type=jnp.float32)
        up_pre = jnp.dot(normed_mlp, w_up, preferred_element_type=jnp.float32)
        gated = (jax.nn.silu(gate_pre) * up_pre).astype(jnp.bfloat16)
        mlp_sum = jnp.zeros((SEQ, D), jnp.float32)
        for index in range(TP):
            partial = jnp.dot(gated[:, index * ff_part:(index + 1) * ff_part], w_down[index * ff_part:(index + 1) * ff_part], preferred_element_type=jnp.float32)
            mlp_sum = mlp_sum + partial.astype(jnp.bfloat16).astype(jnp.float32)
        out_row = (hidden.astype(jnp.float32) + mlp_sum).astype(jnp.bfloat16)
        return out_row, keys, values

    y, new_keys, new_values = lax.map(one_sequence, (x, seq_lens))
    k_cache_out = lax.dynamic_update_slice(k_cache, new_keys, (0, 0, 0, 0))
    v_cache_out = lax.dynamic_update_slice(v_cache, new_values, (0, 0, 0, 0))
    return y, k_cache_out, v_cache_out
```

```python
import functools

import jax
import jax.numpy as jnp
import numpy as np
from jax import lax
from jax.experimental import pallas as pl
from jax.experimental.pallas import tpu as pltpu
from jax.sharding import PartitionSpec as P

EPS = 1e-5
ROPE_BASE = 10000.0
VMEM_LIMIT = 63 * 1024 * 1024
TILE = 256
WIDE = 512
ANY = pl.BlockSpec(memory_space=pltpu.HBM)
ATTN_SEQS = (2, 2, 4)
OUT_PIECES = ((4, 4), (8,), (4, 4))
OUT_TILE = 1024
DOWN_PIECES = ((8, 8), (4, 4, 4, 4))


def kernel_call(kernel, **kwargs):
    return pl.pallas_call(kernel, **kwargs)


def dot32(lhs, rhs):
    return jnp.dot(lhs, rhs, preferred_element_type=jnp.float32)


def params():
    return pltpu.CompilerParams(dimension_semantics=("arbitrary",), vmem_limit_bytes=VMEM_LIMIT)


def once(shape, index=(0, 0)):
    return pl.BlockSpec(shape, lambda j, *_: index, pipeline_mode=pl.Buffered(1))


def attend_kernel(own, tiles_per_kv, first_seq, me_ref, lens_ref, x_ref, gain_ref, cos_ref, sin_ref, wq_ref, wk_ref, wv_ref, *rest):
    o_ref, k_ref, v_ref, normed, wbuf, sems = rest[-6:]
    step = pl.program_id(0)
    steps = pl.num_programs(0)
    me = me_ref[0]
    chunk = x_ref.shape[0]
    seq, head = cos_ref.shape
    seqs = chunk // seq

    def fetch(index, action):
        slot = lax.rem(index, 2)

        @pl.when(index == 0)
        def _():
            getattr(pltpu.make_async_copy(wk_ref, wbuf.at[slot], sems.at[slot]), action)()

        @pl.when(index == 1)
        def _():
            getattr(pltpu.make_async_copy(wv_ref, wbuf.at[slot], sems.at[slot]), action)()

        @pl.when((index >= 2) & (index < steps))
        def _():
            col = pl.multiple_of((index - 2) * TILE, TILE)
            getattr(pltpu.make_async_copy(wq_ref.at[:, pl.ds(col, TILE)], wbuf.at[slot], sems.at[slot]), action)()

    @pl.when(step == 0)
    def _():
        fetch(step, "start")

    fetch(step + 1, "start")

    @pl.when(step == 0)
    def _():
        gain = gain_ref[...].astype(jnp.float32)

        @pl.loop(0, chunk // 16)
        def _(r):
            at = pl.ds(pl.multiple_of(r * 16, 16), 16)
            rows = x_ref[at, :].astype(jnp.float32)
            inv = lax.rsqrt(jnp.mean(rows * rows, axis=-1, keepdims=True) + EPS)
            normed[at, :] = (rows * inv * gain).astype(jnp.bfloat16)

    fetch(step, "wait")

    def turn(vecs):
        even = lax.rem(lax.broadcasted_iota(jnp.int32, vecs.shape, 1), 2) == 0
        partner = jnp.where(even, pltpu.roll(vecs, head - 1, 1), pltpu.roll(vecs, 1, 1))
        return (vecs * cos_ref[...] + partner * sin_ref[...]).astype(jnp.bfloat16)

    proj = dot32(normed[...], wbuf[lax.rem(step, 2)])
    pos = lax.broadcasted_iota(jnp.int32, (seq, 1), 0)

    @pl.when(step == 0)
    def _():
        for s in range(seqs):
            for h in range(TILE // head):
                keys = turn(proj[s * seq:(s + 1) * seq, h * head:(h + 1) * head])
                k_ref[s * seq:(s + 1) * seq, h * head:(h + 1) * head] = jnp.where(pos < lens_ref[first_seq + s], keys, jnp.zeros_like(keys))

    @pl.when(step == 1)
    def _():
        for s in range(seqs):
            values = proj[s * seq:(s + 1) * seq].astype(jnp.bfloat16)
            v_ref[s * seq:(s + 1) * seq, :] = jnp.where(pos < lens_ref[first_seq + s], values, jnp.zeros_like(values))

    @pl.when(step >= 2)
    def _():
        kv_col = pl.multiple_of((step - 2) // tiles_per_kv * head, head)
        row_id = lax.broadcasted_iota(jnp.int32, (seq, seq), 0)
        col_id = lax.broadcasted_iota(jnp.int32, (seq, seq), 1)
        for s in range(seqs):
            at = slice(s * seq, (s + 1) * seq)
            keys = k_ref[at, pl.ds(kv_col, head)]
            values = v_ref[at, pl.ds(kv_col, head)]
            allowed = (col_id <= row_id) & (col_id < lens_ref[first_seq + s])
            for h in range(TILE // head):
                query = turn(proj[at, h * head:(h + 1) * head])
                scores = lax.dot_general(query, keys, (((1,), (1,)), ((), ())), preferred_element_type=jnp.float32) * head ** -0.5
                scores = jnp.where(allowed, scores, -jnp.inf)
                weights = jnp.exp(scores - jnp.max(scores, axis=-1, keepdims=True))
                probs = (weights / jnp.sum(weights, axis=-1, keepdims=True)).astype(jnp.bfloat16)
                mixed = dot32(probs, values).astype(jnp.bfloat16)
                for part in range(seq // own):
                    owner = s * (seq // own) + part
                    row = pl.multiple_of(lax.bitwise_xor(me, owner) * own, own)
                    o_ref[pl.ds(row, own), h * head:(h + 1) * head] = mixed[part * own:(part + 1) * own]


def attend(first_row, chunk, tp_size, me, lens, x_flat, gain, cos_tab, sin_tab, w_query, w_key, w_value, deps=()):
    width = x_flat.shape[1]
    seq, head = cos_tab.shape
    q_cols, kv_cols = w_query.shape[1], w_key.shape[1]
    steps = q_cols // TILE + 2
    x_spec = pl.BlockSpec((pl.Element(chunk), pl.Element(width)), lambda j, *_: (first_row, 0), pipeline_mode=pl.Buffered(1))
    return kernel_call(
        functools.partial(attend_kernel, chunk // tp_size, q_cols // TILE // (kv_cols // head), first_row // seq),
        grid_spec=pltpu.PrefetchScalarGridSpec(
            num_scalar_prefetch=2,
            grid=(steps,),
            in_specs=[x_spec, once((1, width)), once((seq, head)), once((seq, head))] + [ANY] * (3 + len(deps)),
            out_specs=[pl.BlockSpec((chunk, TILE), lambda j, *_: (0, jnp.maximum(j - 2, 0)))] + [pl.BlockSpec((chunk, kv_cols), lambda j, *_: (0, 0))] * 2,
            scratch_shapes=[pltpu.VMEM((chunk, width), jnp.bfloat16), pltpu.VMEM((2, width, TILE), jnp.bfloat16), pltpu.SemaphoreType.DMA((2,))],
        ),
        out_shape=[jax.ShapeDtypeStruct((chunk, q_cols), jnp.bfloat16)] + [jax.ShapeDtypeStruct((chunk, kv_cols), jnp.bfloat16)] * 2,
        compiler_params=params(),
    )(me, lens, x_flat, gain, cos_tab, sin_tab, w_query, w_key, w_value, *deps)


def load_lhs(blocks, lhs, sems, by_rows):
    @pl.when(pl.program_id(0) == 0)
    def _():
        copies, at = [], 0
        for i, block in enumerate(blocks):
            size = block.shape[0 if by_rows else 1]
            target = lhs.at[pl.ds(at, size)] if by_rows else lhs.at[:, pl.ds(at, size)]
            copies.append(pltpu.make_async_copy(block, target, sems.at[i]))
            at += size
        for copy in copies:
            copy.start()
        for copy in copies:
            copy.wait()


def gate_up_kernel(n_blocks, *refs):
    blocks, (wg_ref, wu_ref), (o_ref, lhs, sems) = refs[:n_blocks], refs[n_blocks:n_blocks + 2], refs[-3:]
    load_lhs(blocks, lhs, sems, True)
    gate = dot32(lhs[...], wg_ref[...])
    up = dot32(lhs[...], wu_ref[...])
    o_ref[...] = (gate * jax.nn.sigmoid(gate) * up).astype(jnp.bfloat16)


def gate_up(blocks, w_gate, w_up, first, tiles, deps=()):
    width = blocks[0].shape[1]
    rows = sum(block.shape[0] for block in blocks)
    cols = min(tiles * TILE, w_gate.shape[1] - first * TILE)
    w_spec = pl.BlockSpec((width, TILE), lambda j: (0, first + j))
    return kernel_call(
        functools.partial(gate_up_kernel, len(blocks)),
        grid=(tiles,),
        in_specs=[ANY] * len(blocks) + [w_spec] * 2 + [ANY] * len(deps),
        out_specs=pl.BlockSpec((rows, TILE), lambda j: (0, j)),
        out_shape=jax.ShapeDtypeStruct((rows, cols), jnp.bfloat16),
        scratch_shapes=[pltpu.VMEM((rows, width), jnp.bfloat16), pltpu.SemaphoreType.DMA((len(blocks),))],
        compiler_params=params(),
    )(*blocks, w_gate, w_up, *deps)


def project_kernel(n_blocks, n_outs, *refs):
    blocks, w_ref = refs[:n_blocks], refs[n_blocks]
    outs, lhs, sems = refs[-2 - n_outs:-2], refs[-2], refs[-1]
    load_lhs(blocks, lhs, sems, False)
    partial = dot32(lhs[...], w_ref[...]).astype(jnp.bfloat16)
    own = outs[0].shape[0]
    for k, out in enumerate(outs):
        out[...] = partial[k * own:(k + 1) * own]


def project(blocks, weight, tile, first, tiles, n_outs, deps=()):
    rows = blocks[0].shape[0]
    depth = weight.shape[0]
    own = rows // n_outs
    return kernel_call(
        functools.partial(project_kernel, len(blocks), n_outs),
        grid=(tiles,),
        in_specs=[ANY] * len(blocks) + [pl.BlockSpec((depth, tile), lambda j: (0, first + j))] + [ANY] * len(deps),
        out_specs=[pl.BlockSpec((own, tile), lambda j: (0, j))] * n_outs,
        out_shape=[jax.ShapeDtypeStruct((own, tiles * tile), jnp.bfloat16)] * n_outs,
        scratch_shapes=[pltpu.VMEM((rows, depth), jnp.bfloat16), pltpu.SemaphoreType.DMA((len(blocks),))],
        compiler_params=params(),
    )(*blocks, weight, *deps)


def add_norm_kernel(n_pieces, n_parts, *refs):
    pieces = [refs[p * n_parts:(p + 1) * n_parts] for p in range(n_pieces)]
    x_ref, gain_ref = refs[n_pieces * n_parts:n_pieces * n_parts + 2]
    h_ref, n_ref, h32 = refs[-3:]
    col = 0
    square = jnp.zeros((h_ref.shape[0], 1), jnp.float32)
    for parts in pieces:
        at = slice(col, col + parts[0].shape[1])
        total = parts[0][...].astype(jnp.float32)
        for part in parts[1:]:
            total = total + part[...].astype(jnp.float32)
        hidden = (x_ref[:, at].astype(jnp.float32) + total).astype(jnp.bfloat16)
        h_ref[:, at] = hidden
        hidden = hidden.astype(jnp.float32)
        h32[:, at] = hidden
        square = square + jnp.sum(hidden * hidden, axis=-1, keepdims=True)
        col += parts[0].shape[1]
    inv = lax.rsqrt(square / h_ref.shape[1] + EPS)
    n_ref[...] = (h32[...] * inv * gain_ref[...].astype(jnp.float32)).astype(jnp.bfloat16)


def add_norm(pieces, row_block, x_flat, gain, hidden, hidden_rows, hidden_first, deps=()):
    n_parts = len(pieces[0])
    own = pieces[0][0].shape[0]
    width = x_flat.shape[1]
    flat = [part for parts in pieces for part in parts]
    n_in = len(flat) + 2
    step_rows = 32
    steps = own // step_rows
    extra = (() if hidden is None else (hidden,)) + tuple(deps)

    def kernel(*refs):
        add_norm_kernel(len(pieces), n_parts, *refs[1:1 + n_in], *refs[1 + n_in + len(extra):])

    return kernel_call(
        kernel,
        grid_spec=pltpu.PrefetchScalarGridSpec(
            num_scalar_prefetch=1,
            grid=(steps,),
            in_specs=[pl.BlockSpec((step_rows, part.shape[1]), lambda j, *_: (j, 0)) for part in flat]
            + [pl.BlockSpec((step_rows, width), lambda j, at: (at[0] + j, 0)), once((1, width))] + [ANY] * len(extra),
            out_specs=[pl.BlockSpec((step_rows, width), lambda j, *_: (hidden_first // step_rows + j, 0)), pl.BlockSpec((step_rows, width), lambda j, *_: (j, 0))],
            scratch_shapes=[pltpu.VMEM((step_rows, width), jnp.float32)],
        ),
        out_shape=[jax.ShapeDtypeStruct((hidden_rows, width), jnp.bfloat16), jax.ShapeDtypeStruct((own, width), jnp.bfloat16)],
        input_output_aliases={} if hidden is None else {1 + n_in: 0},
        compiler_params=params(),
    )(row_block * steps, *flat, x_flat, gain, *extra)


def hold(arrays, deps):
    def kernel(*refs):
        pass

    return kernel_call(
        kernel,
        in_specs=[ANY] * (len(arrays) + len(deps)),
        out_specs=[ANY] * len(arrays),
        out_shape=[jax.ShapeDtypeStruct(a.shape, a.dtype) for a in arrays],
        input_output_aliases={i: i for i in range(len(arrays))},
    )(*arrays, *deps)


def add_rows(parts, hidden, first_col, deps=()):
    own, cols = parts[0].shape
    step_rows = 64

    def kernel(*refs):
        total = refs[0][...].astype(jnp.float32)
        for ref in refs[1:len(parts)]:
            total = total + ref[...].astype(jnp.float32)
        refs[-1][...] = (refs[len(parts)][...].astype(jnp.float32) + total).astype(jnp.bfloat16)

    spec = pl.BlockSpec((step_rows, cols), lambda i: (i, 0))
    return kernel_call(
        kernel,
        grid=(own // step_rows,),
        in_specs=[spec] * len(parts) + [pl.BlockSpec((step_rows, cols), lambda i: (i, first_col // cols))] + [ANY] * len(deps),
        out_specs=spec,
        out_shape=jax.ShapeDtypeStruct((own, cols), jnp.bfloat16),
        compiler_params=params(),
    )(*parts, hidden, *deps)


def place_rows(me, y, shape, blocks, row_block, first_col, part, deps=()):
    parts = blocks[0].shape[0] // part
    cols = blocks[0].shape[1]

    def kernel(*refs):
        for k in range(len(blocks)):
            @pl.when(pl.program_id(0) == k)
            def _():
                refs[-2][...] = refs[1 + k][...]

        refs[-1][...] = jnp.zeros_like(refs[-1])

    block = (part, cols)
    return kernel_call(
        kernel,
        grid_spec=pltpu.PrefetchScalarGridSpec(
            num_scalar_prefetch=1,
            grid=(len(blocks), parts),
            in_specs=[pl.BlockSpec(block, lambda b, i, me, k=k: (jnp.where(b == k, i, jnp.where(b < k, 0, parts - 1)), 0)) for k in range(len(blocks))] + [ANY] * (len(deps) + (y is not None)),
            out_specs=[pl.BlockSpec(block, lambda b, i, me: (row_block(lax.bitwise_xor(me[0], b), i), first_col // cols)), pl.BlockSpec((8, 128), lambda *_: (0, 0))],
        ),
        out_shape=[jax.ShapeDtypeStruct(shape, jnp.bfloat16), jax.ShapeDtypeStruct((8, 128), jnp.float32)],
        input_output_aliases={} if y is None else {1 + len(blocks): 0},
        compiler_params=pltpu.CompilerParams(dimension_semantics=("arbitrary",) * 2, vmem_limit_bytes=VMEM_LIMIT),
    )(me, *blocks, *(() if y is None else (y,)), *deps)


def rotary_tables(seq_len, head_dim):
    inv_freq = np.float32(ROPE_BASE) ** (-np.arange(0, head_dim, 2, dtype=np.float32) / np.float32(head_dim))
    angles = (np.arange(seq_len, dtype=np.float32)[:, None] * inv_freq[None, :].astype(np.float32)).astype(np.float64)
    sign = np.where(np.arange(head_dim) % 2 == 0, -1.0, 1.0)[None, :]
    return np.repeat(np.cos(angles), 2, axis=1).astype(np.float32), (np.repeat(np.sin(angles), 2, axis=1) * sign).astype(np.float32)


def solution(mesh):
    tp_size = mesh.shape["tp"]

    def swap(block, mask):
        return lax.ppermute(block, "tp", [(s, s ^ mask) for s in range(tp_size)])

    def exchange(pieces):
        return [pieces[0]] + [swap(pieces[k], k) for k in (2, 3, 1)]

    def send(block):
        return block, swap(block, 1), swap(block, 2)

    def forward(sent, deps):
        block, from_core, from_chip = sent
        from_chip = hold([from_chip], deps)[0]
        return [block, from_core, from_chip, swap(from_chip, 1)]

    def layer_body(x, seq_lens, w_query, w_key, w_value, w_out, w_gate, w_up, w_down, attn_gain, mlp_gain, k_cache, v_cache):
        batch_size, seq_len, width = x.shape
        head_dim = k_cache.shape[3]
        rows = batch_size * seq_len
        x_flat = x.reshape(rows, width)
        me = lax.axis_index("tp").astype(jnp.int32).reshape(1)
        cos_tab, sin_tab = (jnp.asarray(t) for t in rotary_tables(seq_len, head_dim))
        gain1, gain2 = attn_gain.reshape(1, width), mlp_gain.reshape(1, width)
        starts = [sum(ATTN_SEQS[:c]) * seq_len for c in range(len(ATTN_SEQS))]
        sizes = [n * seq_len for n in ATTN_SEQS]
        owns = [n // tp_size for n in sizes]

        def attn(c, deps=()):
            return attend(starts[c], sizes[c], tp_size, me, seq_lens, x_flat, gain1, cos_tab, sin_tab, w_query, w_key, w_value, deps)

        def pieces_of(lhs, weight, tile, tiles, deps=()):
            out, first = [], 0
            for n in tiles:
                out.append(project(lhs, weight, tile, first, n, tp_size, deps))
                deps = (out[-1][0],)
                first += n
            return out

        def out_proj(c, lhs, deps=()):
            return pieces_of([lhs], w_out, OUT_TILE, OUT_PIECES[c], deps)

        def norm(c, received, hidden, hidden_rows, hidden_first, deps):
            return add_norm(received, starts[c] // owns[c] + me, x_flat, gain2, hidden, hidden_rows, hidden_first, deps)

        o0, k0, v0 = attn(0)
        p0 = out_proj(0, o0)
        r0 = [exchange(p) for p in p0]
        o1, k1, v1 = attn(1, (p0[-1][0],))
        h0, n0 = norm(0, r0, None, owns[0] + owns[1], 0, (o1,))
        g0 = send(n0)
        p1 = out_proj(1, o1, (n0,))
        r1 = [exchange(p) for p in p1]
        o2, k2, v2 = attn(2, (p1[-1][0],))
        h0, n1 = norm(1, r1, h0, owns[0] + owns[1], owns[0], (o2,))
        g1 = send(n1)
        g0 = forward(g0, (n1,))
        p2 = out_proj(2, o2, (g0[2],))
        r2 = [exchange(p) for p in p2]
        g1 = forward(g1, (p2[-1][0],))
        lhs0 = [g[k] for k in range(tp_size) for g in (g0, g1)]
        all_tiles = -(-w_gate.shape[1] // TILE)
        half = all_tiles // 2
        u0 = [gate_up(lhs0, w_gate, w_up, 0, all_tiles, (g1[2],))]
        h1, n2 = norm(2, r2, None, owns[2], 0, (u0[0],))
        g2 = send(n2)
        d0 = pieces_of(u0, w_down, WIDE, DOWN_PIECES[0], (n2,))
        s0 = [exchange(p) for p in d0]
        g2 = forward(g2, (d0[-1][0],))
        u1 = [gate_up(g2, w_gate, w_up, 0, half, (g2[2],))]

        def add(c, i, received, hidden, deps):
            first = sum(DOWN_PIECES[c][:i]) * WIDE
            return add_rows(received[i], hidden, first, deps)

        a00 = add(0, 0, s0, h0, (u1[0],))
        e00 = send(a00)
        u1.append(gate_up(g2, w_gate, w_up, half, all_tiles - half, (a00,)))
        a01 = add(0, 1, s0, h0, (u1[1],))
        e01 = send(a01)
        d1 = pieces_of(u1, w_down, WIDE, DOWN_PIECES[1], (a01,))
        s1 = [exchange(p) for p in d1]

        def row_block(c):
            return (lambda owner, i: tp_size * i + owner) if c == 0 else (lambda owner, i: starts[2] // owns[2] + owner)

        def place(c, i, y, blocks, deps):
            first = sum(DOWN_PIECES[c][:i]) * WIDE
            return place_rows(me, y, (rows, width), blocks, row_block(c), first, owns[0] if c == 0 else owns[2], deps)

        def cache_of(cache, blocks):
            new_rows = jnp.concatenate(blocks, axis=0).reshape(batch_size, seq_len, -1, head_dim)
            return jnp.concatenate([new_rows, cache[:, seq_len:]], axis=1)

        k_out, v_out = cache_of(k_cache, [k0, k1, k2]), cache_of(v_cache, [v0, v1, v2])
        b00 = forward(e00, (d1[-1][0],))
        a10 = add(1, 0, s1, h1, (b00[2],))
        e10 = send(a10)
        b01 = forward(e01, (a10,))
        a11 = add(1, 1, s1, h1, (b01[2],))
        e11 = send(a11)
        y, token = place(0, 0, None, b00, (a11,))
        b10 = forward(e10, (token, k_out, v_out))
        a12 = add(1, 2, s1, h1, (b10[2],))
        e12 = send(a12)
        y, token = place(0, 1, y, b01, (a12,))
        b11 = forward(e11, (token,))
        y, token = place(1, 0, y, b10, (b11[2],))
        a13 = add(1, 3, s1, h1, (token,))
        e13 = send(a13)
        y, token = place(1, 1, y, b11, (a13,))
        b12 = forward(e12, (token,))
        b13 = forward(e13, (b12[2],))
        y, token = place(1, 2, y, b12, (b13[2],))
        y, token = place(1, 3, y, b13, ())

        return y.reshape(x.shape), k_out, v_out

    cache_spec = P("dp", None, "tp", None)
    return jax.shard_map(layer_body, mesh=mesh, in_specs=(P("dp", None, None), P("dp"), P(None, "tp"), P(None, "tp"), P(None, "tp"), P("tp", None), P(None, "tp"), P(None, "tp"), P("tp", None), P(), P(), cache_spec, cache_spec), out_specs=(P("dp", None, None), cache_spec, cache_spec), check_vma=False)
```
